32 devices in a mesh: grp: 2 (over y), seq: 4 (over z), head: 2 (over x), batch: 2 (over core).
Axes of the slice: x: 2, y: 2, z: 4, core: 2. Of those that a mesh axis runs over, the one named last changes fastest.
Arguments:
- queries: bfloat16 [64, 64, 128], P(('grp', 'batch'), 'head'), parts along dimension 0, may hold values from -8 to 8
- key_cache: bfloat16 [64, 8, 1024, 128], P(('grp', 'batch'), 'head', 'seq'), parts along dimension 0, may hold values from -5 to 5
- value_cache: bfloat16 [64, 8, 1024, 128], P(('grp', 'batch'), 'head', 'seq'), parts along dimension 0, may hold values from -5 to 5
- gate_logits: float32 [2, 64, 64], P(None, ('grp', 'batch'), 'head'), parts along dimension 1, may hold values from -6 to 6
- lengths: int32 [64], P(('grp', 'batch')), parts along dimension 0, may hold values from 256 to 1024, as said below
- chosen: int32 [64, 8, 2], P(('grp', 'batch'), 'head'), parts along dimension 0, may hold values from 0 to 7, as said below
- counts: int32 [64, 8], P(('grp', 'batch'), 'head'), parts along dimension 0, may hold values from 1 to 2, as said below
Outputs:
- output: bfloat16 [64, 64, 128], P(('grp', 'batch'), 'head'), parts along dimension 0
The draws below stay inside these ranges and needn't reach their ends.
There are 2 independent parts, one for each index of `grp`. The reference program is written for one: setup_inputs(seed, part) draws one part's arguments, and reference() takes and returns one part's arrays. A program takes and returns all parts, laid end to end along the dimension named above; each array names one. Nothing has to cross between parts.
Inputs may be any that keep to these rules, and one draw needn't show every extreme that they name: `lengths`: every draw has a sequence of the full length 1024. `chosen`: for each sequence and key-value head the first counts entries are distinct blocks that start below the sequence's length, and the first entry is block 0; the entries after them are ignored. `counts`: every draw has a sequence with 2 valid entries for every key-value head.
All inputs are finite; a program needn't handle non-finite values.
Results may differ from the reference program's by a relative error of at most 0.02.
Values may be sent and summed in bfloat16 or wider, within the bound.
A program may use at most 64 MiB of HBM per device.

```python
import math
import jax
import jax.numpy as jnp
from jax import lax

D_HEAD = 128
Q_HEADS = 64
KV_HEADS = 8
BLOCK = 128
SEQS = 32
BLOCKS = 8
CTX = 1024
TOPK = 2


def plan_draw(key):
    key_lengths = jax.random.fold_in(key, 11)
    key_scores = jax.random.fold_in(key, 12)
    key_counts = jax.random.fold_in(key, 13)
    key_longest = jax.random.fold_in(key, 14)
    lengths = jax.random.randint(key_lengths, (SEQS,), TOPK * BLOCK, CTX + 1, dtype=jnp.int32)
    longest = jax.random.randint(key_longest, (), 0, SEQS, dtype=jnp.int32)
    seq_ids = jnp.arange(SEQS, dtype=jnp.int32)
    lengths = jnp.where(seq_ids == longest, CTX, lengths).astype(jnp.int32)
    valid_blocks = (lengths + BLOCK - 1) // BLOCK
    block_ids = jnp.arange(BLOCKS, dtype=jnp.int32)
    raw_scores = jax.random.randint(key_scores, (SEQS, KV_HEADS, BLOCKS), 0, 1 << 16, dtype=jnp.int32)
    block_score = raw_scores * BLOCKS + block_ids[None, None, :]
    block_score = jnp.where(block_ids[None, None, :] < valid_blocks[:, None, None], block_score, -1 - block_ids[None, None, :])
    block_score = jnp.where(block_ids[None, None, :] == 0, 1 << 29, block_score)
    chosen = lax.top_k(block_score, TOPK)[1].astype(jnp.int32)
    counts = jax.random.randint(key_counts, (SEQS, KV_HEADS), 1, TOPK + 1, dtype=jnp.int32)
    counts = jnp.where((seq_ids == longest)[:, None], TOPK, counts).astype(jnp.int32)
    return (lengths, chosen, counts)


def draw_lengths(key, part):
    return plan_draw(key)[0]


def draw_chosen(key, part):
    return plan_draw(key)[1]


def draw_counts(key, part):
    return plan_draw(key)[2]


def draw_queries(key, part):
    full_shape = (SEQS, Q_HEADS, D_HEAD)
    drawn = jnp.clip(2.5 * jax.random.normal(jax.random.fold_in(key, 42), full_shape, jnp.float32), -8.0, 8.0)
    return drawn.astype(jnp.bfloat16)


def draw_key_cache(key, part):
    first_shape = (SEQS, KV_HEADS, BLOCK, D_HEAD)
    rest_shape = (SEQS, KV_HEADS, CTX - BLOCK, D_HEAD)
    first_rows = jnp.clip(jax.random.normal(jax.random.fold_in(key, 34), first_shape, jnp.float32), -5.0, 5.0)
    rest_rows = jnp.clip(jax.random.normal(jax.random.fold_in(key, 35), rest_shape, jnp.float32), -5.0, 5.0)
    return jnp.concatenate([first_rows, rest_rows], axis=2).astype(jnp.bfloat16)


def steps_of(key, extent, shards, low, top_value):
    loudness, own = 1.0, jax.random.fold_in(key, 6)
    for dim, blocks in shards:
        draws = jnp.exp(jax.random.uniform(jax.random.fold_in(own, dim), (blocks,), jnp.float32, low / len(shards), top_value / len(shards)))
        loudness = loudness * jnp.repeat(draws, extent[dim] // blocks).reshape([-1 if axis == dim else 1 for axis in range(len(extent))])
    return loudness


def noise(rng, dims, scale, limit, pieces=(), held_as=jnp.bfloat16):
    values = jax.random.normal(rng, dims, jnp.float32) * scale
    if len(pieces) > 0:
        values = steps_of(rng, dims, pieces, -0.22, 0.18) * values
    return jnp.clip(values, min=-limit, max=limit).astype(held_as)


def setup_inputs(seed: int = 0, part: int = 0) -> dict:
    key_list = jax.random.split(jax.random.key(seed), 8)
    part_splits = jax.random.split(jax.random.fold_in(key_list[7], part), 8)
    return {
        "queries": draw_queries(jax.random.fold_in(jax.random.fold_in(key_list[7], part), 71), part),
        "key_cache": draw_key_cache(jax.random.fold_in(jax.random.fold_in(key_list[7], part), 71), part),
        "value_cache": noise(part_splits[2], (SEQS, KV_HEADS, CTX, D_HEAD), 1.0, 5.0, ((0, 2), (1, 2), (2, 4))),
        "gate_logits": noise(part_splits[3], (2, SEQS, Q_HEADS), 1.5, 6.0, ((1, 2), (2, 2)), jnp.float32),
        "lengths": draw_lengths(jax.random.fold_in(jax.random.fold_in(key_list[7], part), 71), part),
        "chosen": draw_chosen(jax.random.fold_in(jax.random.fold_in(key_list[7], part), 71), part),
        "counts": draw_counts(jax.random.fold_in(jax.random.fold_in(key_list[7], part), 71), part),
    }


def attend(query_rows, key_rows, value_rows, live_mask, score_scale):
    scores = jnp.einsum('hgd,hnd->hgn', query_rows, key_rows, precision=lax.Precision.HIGHEST) * score_scale
    scores = jnp.where(live_mask[:, None, :], scores, -1e+30)
    row_max = lax.optimization_barrier(jnp.max(scores, axis=2, keepdims=True))
    weights = jnp.where(live_mask[:, None, :], jnp.exp(scores - row_max), 0.0)
    weight_sum = lax.optimization_barrier(jnp.sum(weights, axis=2, keepdims=True))
    rounded = lax.optimization_barrier(weights.astype(jnp.bfloat16)).astype(jnp.float32)
    summed = jnp.einsum('hgn,hnd->hgd', rounded, value_rows, precision=lax.Precision.HIGHEST)
    return summed / weight_sum

def pool_rows(rows_float, head_count, block_count, head_width, root_fill):
    summed = lax.optimization_barrier(jnp.sum(rows_float.reshape(head_count, block_count, BLOCK, head_width), axis=2)) / root_fill
    return lax.optimization_barrier(summed.astype(jnp.bfloat16)).astype(jnp.float32)

def one_sequence(sequence):
    query_in, key_rows, value_rows, gate_row, length, chosen_row, live_slots = sequence
    head_count, context, head_width = key_rows.shape
    group_size = query_in.shape[0] // head_count
    block_count = context // BLOCK
    score_scale = 1.0 / math.sqrt(head_width)
    query_rows = query_in.reshape(head_count, group_size, head_width).astype(jnp.float32)
    position = jnp.arange(context, dtype=jnp.int32)
    live_mask = position < length
    key_float = jnp.where(live_mask[None, :, None], key_rows.astype(jnp.float32), 0.0)
    value_float = jnp.where(live_mask[None, :, None], value_rows.astype(jnp.float32), 0.0)
    starts = jnp.arange(block_count, dtype=jnp.int32) * BLOCK
    filled = jnp.clip(length - starts, 0, BLOCK)
    root_fill = jnp.sqrt(jnp.maximum(filled, 1).astype(jnp.float32))[None, :, None]
    pooled_keys = pool_rows(key_float, head_count, block_count, head_width, root_fill)
    pooled_values = pool_rows(value_float, head_count, block_count, head_width, root_fill)
    block_live = jnp.broadcast_to((filled > 0)[None, :], (head_count, block_count))
    compressed = attend(query_rows, pooled_keys, pooled_values, block_live, score_scale)
    slot_live = jnp.arange(chosen_row.shape[1], dtype=jnp.int32)[None, :] < live_slots[:, None]
    block_ids = jnp.arange(block_count, dtype=jnp.int32)
    picked = jnp.any((chosen_row[:, :, None] == block_ids[None, None, :]) & slot_live[:, :, None], axis=1)
    token_mask = live_mask[None, :] & jnp.repeat(picked, BLOCK, axis=1)
    selected = attend(query_rows, key_float, value_float, token_mask, score_scale)
    gate_pair = jax.nn.sigmoid(gate_row).reshape(2, head_count, group_size, 1)
    mixed = gate_pair[0] * compressed + gate_pair[1] * selected
    return mixed.reshape(head_count * group_size, head_width).astype(jnp.bfloat16)

def reference(queries, key_cache, value_cache, gate_logits, lengths, chosen, counts):
    gate_rows = jnp.moveaxis(gate_logits, 0, 1)
    return lax.map(one_sequence, (queries, key_cache, value_cache, gate_rows, lengths, chosen, counts))
```

```python
import functools
import math

import jax
import jax.numpy as jnp
from jax import lax
from jax.experimental import pallas as pl
from jax.experimental.pallas import tpu as pltpu
from jax.sharding import PartitionSpec as P

BLOCK = 128
LANES = 128
ROWS = 8
NEG = -1e30
MESH = pl.DeviceIdType.MESH


def owners_of(n, chunks):
    if chunks >= 2 * n and n >= 3:
        return [0, 0] + [2 - c % 2 for c in range(chunks - 3)] + [0]
    return [c * n // chunks for c in range(chunks)]


def plan_of(n, pairs, group):
    size = min(pairs, LANES // group)
    parts = pairs // size
    cuts = max(2, n // parts)
    return size, parts, cuts


def kernel(
    n, q_ref, k_hbm, v_hbm, gate_ref, len_ref, chosen_ref, count_ref, o_ref,
    k_buf, v_buf, msg, r_msg, gates,
    k_sem, v_sem, ms_sem, mr_sem, gs_sem, gr_sem,
):
    pairs, tokens, width = k_hbm.shape
    group = q_ref.shape[0] // pairs
    blocks = tokens // BLOCK
    heads = count_ref.shape[0]
    slots = chosen_ref.shape[1]
    size, parts, cuts = plan_of(n, pairs, group)
    own = size // cuts
    chunks = parts * cuts
    owners = owners_of(n, chunks)
    holders = sorted(set(owners))
    owned = {o: [c for c in range(chunks) if owners[c] == o] for o in holders}
    most = max(len(v) for v in owned.values())
    span = own * group
    pooled_rows = -(-own * blocks // ROWS) * ROWS
    stat_at = span + pooled_rows
    per_tile = ROWS // blocks
    scale = 1.0 / math.sqrt(width)
    me = lax.axis_index("seq")

    def load(k, hbm, buf, sem):
        return pltpu.make_async_copy(hbm.at[pl.ds(k * size, size)], buf.at[k], sem.at[k])

    for k in range(parts):
        load(k, k_hbm, k_buf, k_sem).start()
        load(k, v_hbm, v_buf, v_sem).start()

    barrier = pltpu.get_barrier_semaphore()
    holds = functools.reduce(jnp.logical_or, [me == o for o in holders])

    @pl.when(holds)
    def _():
        for r in range(1, n):
            pl.semaphore_signal(
                barrier, inc=1, device_id={"seq": lax.rem(me + r, n)}, device_id_type=MESH
            )

    lane = lax.broadcasted_iota(jnp.int32, (ROWS, LANES), 1)
    row = lax.broadcasted_iota(jnp.int32, (ROWS, LANES), 0)
    lane_pair = lax.div(lane, group)
    token = lax.broadcasted_iota(jnp.int32, (BLOCK, LANES), 0)

    def gate_row(branch, first):
        pieces = []
        at = first
        while at < first + own:
            b, h = divmod(at, heads)
            run = min(heads - h, first + own - at)
            pieces.append(gate_ref[branch, b : b + 1, h * group : (h + run) * group])
            at += run
        if span < LANES:
            pieces.append(jnp.zeros((1, LANES - span), jnp.float32))
        return jax.nn.sigmoid(jnp.concatenate(pieces, axis=1))

    for c in range(chunks):
        gates[c] = jnp.where(row == 0, gate_row(1, c * own), gate_row(0, c * own))

    def send(c):
        slot = lax.rem(me - owners[c] + n, n) - 1
        at = owned[owners[c]].index(c)
        return pltpu.make_async_remote_copy(
            src_ref=msg.at[c], dst_ref=r_msg.at[at, slot],
            send_sem=ms_sem.at[c], recv_sem=mr_sem.at[at, slot],
            device_id={"seq": owners[c]}, device_id_type=MESH,
        )

    def arrival(at, slot):
        return pltpu.make_async_remote_copy(
            src_ref=msg.at[0], dst_ref=r_msg.at[at, slot],
            send_sem=ms_sem.at[0], recv_sem=mr_sem.at[at, slot],
            device_id={"seq": lax.rem(me + 1 + slot, n)}, device_id_type=MESH,
        )

    def spread(values):
        line = jnp.full((1, LANES), values[0], jnp.int32)
        for i in range(1, size):
            line = jnp.where(lane_pair[:1] == i, values[i], line)
        return line

    def part(k):
        first = k * size
        ids = [divmod(first + i, heads) for i in range(size)]
        lengths = [len_ref[b] for b, _ in ids]
        length_line = spread(lengths)
        count_line = spread([count_ref[h, b] for b, h in ids])
        chosen_lines = [spread([chosen_ref[h, slot, b] for b, h in ids]) for slot in range(slots)]
        chosen_lines = [jnp.where(slot < count_line, line, -1) for slot, line in enumerate(chosen_lines)]

        rows = q_ref[first * group : (first + size) * group, :].astype(jnp.float32)
        if size * group < LANES:
            rows = jnp.concatenate([rows, jnp.zeros((LANES - size * group, width), jnp.float32)], axis=0)
        columns = rows.T
        load(k, k_hbm, k_buf, k_sem).wait()
        scores = None
        for i in range(0, size, 2):
            both = range(i, min(i + 2, size))
            held = jnp.concatenate(
                [jnp.where(lane_pair[:1] == p, columns, 0.0) for p in both], axis=0
            ).astype(jnp.bfloat16)
            keys = jnp.concatenate([k_buf[k, p] for p in both], axis=1)
            product = jnp.dot(keys, held, preferred_element_type=jnp.float32)
            scores = product if scores is None else scores + product
        scores = scores * scale

        stats = jnp.full((ROWS, LANES), NEG, jnp.float32)
        masked, inside = [], []
        for j in range(blocks):
            block = me * blocks + j
            filled = jnp.clip(length_line - block * BLOCK, 0, BLOCK)
            hits = [line == block for line in chosen_lines]
            limit = jnp.where(functools.reduce(jnp.logical_or, hits), filled, 0)
            block_scores = scores[j * BLOCK : (j + 1) * BLOCK]
            root = lax.rsqrt(jnp.maximum(filled, 1).astype(jnp.float32))
            total = jnp.sum(jnp.where(token < filled, block_scores, 0.0), axis=0, keepdims=True)
            stats = jnp.where(row == 1 + j, jnp.where(filled > 0, total * root, NEG), stats)
            inside.append(token < limit)
            masked.append(jnp.where(inside[j], block_scores, NEG))
        top = jnp.max(functools.reduce(jnp.maximum, masked), axis=0, keepdims=True)
        weights = [jnp.where(i, jnp.exp(m - top), 0.0) for i, m in zip(inside, masked)]
        weight_sum = jnp.sum(functools.reduce(jnp.add, weights), axis=0, keepdims=True)
        safe_sum = jnp.maximum(weight_sum, 1.0)
        log_sum = jnp.where(weight_sum > 0.0, top + jnp.log(safe_sum), NEG)
        stats = jnp.where(row == 0, log_sum, stats)
        high = stats.astype(jnp.bfloat16).astype(jnp.float32)
        low = stats - high
        half = ROWS // 2
        parted = jnp.concatenate([high[:half], low[:half]], axis=0)
        inverse = 1.0 / safe_sum
        weight_rows = jnp.concatenate([(w * inverse).T for w in weights], axis=1)

        load(k, v_hbm, v_buf, v_sem).wait()
        for cut in range(cuts):
            c = k * cuts + cut
            outs, tiles = [], []
            for i in range(cut * own, (cut + 1) * own):
                at = (i - cut * own) % per_tile
                if at == 0:
                    members = range(i, min(i + per_tile, (cut + 1) * own))
                    length_rows = jnp.zeros((ROWS, LANES), jnp.int32)
                    for m, p in enumerate(members):
                        length_rows = jnp.where(lax.div(row, blocks) == m, lengths[p], length_rows)
                    start_rows = (me * blocks + lax.rem(row, blocks)) * BLOCK
                    filled_rows = jnp.clip(length_rows - start_rows, 0, BLOCK)
                    root_rows = lax.rsqrt(jnp.maximum(filled_rows, 1).astype(jnp.float32))
                    live = lane < filled_rows
                    pooled = jnp.zeros((ROWS, width), jnp.float32)
                live_rows = jnp.concatenate(
                    [jnp.where(live & (row == at * blocks + j), 1.0, 0.0) for j in range(blocks)], axis=1
                )
                left = jnp.concatenate([weight_rows[i * group : (i + 1) * group], live_rows], axis=0)
                summed = jnp.dot(left.astype(jnp.bfloat16), v_buf[k, i], preferred_element_type=jnp.float32)
                outs.append(summed[:group])
                pooled = pooled + summed[group:]
                if at == per_tile - 1 or i == (cut + 1) * own - 1:
                    tiles.append(pooled * root_rows)
            turned = parted
            if cut:
                turned = pltpu.roll(parted, LANES - cut * span, 1)
            msg[c] = jnp.concatenate(outs + tiles + [turned], axis=0).astype(jnp.bfloat16)

        if k == 0:
            pl.semaphore_wait(barrier, jnp.where(holds, len(holders) - 1, len(holders)))

        for cut in range(cuts):
            c = k * cuts + cut

            @pl.when(me != owners[c])
            def _(c=c):
                send(c).start()

    for k in range(parts):
        part(k)

    def pick(at):
        c = 0
        for o in holders:
            if at < len(owned[o]):
                c = jnp.where(me == o, owned[o][at], c)
        return c

    def has(at):
        return functools.reduce(jnp.logical_or, [me == o for o in holders if at < len(owned[o])])

    def spot(c):
        return pl.ds(pl.multiple_of(c * span, span), span)

    def share(at, r):
        rows = o_ref.at[spot(pick(at))]
        return pltpu.make_async_remote_copy(
            src_ref=rows, dst_ref=rows, send_sem=gs_sem.at[at, r - 1], recv_sem=gr_sem.at[pick(at)],
            device_id={"seq": lax.rem(me + r, n)}, device_id_type=MESH,
        )

    def finish(at):
        c = pick(at)
        for slot in range(n - 1):
            arrival(at, slot).wait_recv()
        half = ROWS // 2
        halves = row[:half]
        parts_in = [r_msg.at[at, slot] for slot in range(n - 1)] + [msg.at[c]]
        all_stats = []
        for ref in parts_in:
            parted = ref[stat_at : stat_at + ROWS, :].astype(jnp.float32)
            all_stats.append(parted[:half] + parted[half:])
        top = functools.reduce(jnp.maximum, all_stats)
        block_row = (halves >= 1) & (halves <= blocks)
        block_top = jnp.max(jnp.where(block_row, top, NEG), axis=0, keepdims=True)
        top = jnp.where(halves == 0, top, block_top)
        shares = [jnp.where(halves <= blocks, jnp.exp(s - top), 0.0) for s in all_stats]
        total = functools.reduce(jnp.add, shares)
        block_total = jnp.sum(jnp.where(block_row, total, 0.0), axis=0, keepdims=True)
        factor = gates[c][:half] / jnp.where(halves == 0, total, block_total)
        wide = lax.broadcasted_iota(jnp.int32, (span, LANES), 1)
        tall = lax.broadcasted_iota(jnp.int32, (span, LANES), 0)
        pool_lane = lax.broadcasted_iota(jnp.int32, (pooled_rows, LANES), 1)
        pool_row = lax.broadcasted_iota(jnp.int32, (pooled_rows, LANES), 0)
        mine = lax.div(pool_lane, group) == lax.div(pool_row, blocks)
        out = None
        for ref, s in zip(parts_in, shares):
            factors = s * factor
            pick_rows = jnp.where(wide == tall, factors[:1], 0.0)
            level = jnp.broadcast_to(factors[1:2], (pooled_rows, LANES))
            for j in range(1, blocks):
                level = jnp.where(lax.rem(pool_row, blocks) == j, factors[1 + j : 2 + j], level)
            level = jnp.where(mine, level, 0.0)
            left = jnp.concatenate([pick_rows, level], axis=0).astype(jnp.bfloat16)[:, :span]
            term = lax.dot_general(
                left, ref[:stat_at, :], (((0,), (0,)), ((), ())), preferred_element_type=jnp.float32
            )
            out = term if out is None else out + term
        o_ref[spot(c), :] = out.astype(jnp.bfloat16)
        for r in range(n - 1, 0, -1):
            share(at, r).start()

    for at in range(most):

        @pl.when(has(at))
        def _(at=at):
            finish(at)

    for c in range(chunks):

        @pl.when(me != owners[c])
        def _(c=c):
            send(c).wait_send()

    for c in range(chunks):

        @pl.when(me != owners[c])
        def _(c=c):
            rows = o_ref.at[c * span : (c + 1) * span]
            pltpu.make_async_remote_copy(
                src_ref=rows, dst_ref=rows, send_sem=gs_sem.at[0, 0], recv_sem=gr_sem.at[c],
                device_id={"seq": owners[c]}, device_id_type=MESH,
            ).wait_recv()

    for at in range(most):

        @pl.when(has(at))
        def _(at=at):
            for r in range(1, n):
                share(at, r).wait_send()


def on_device(n, queries, key_cache, value_cache, gate_logits, lengths, chosen, counts):
    batch_rows, head_count, context, width = key_cache.shape
    pairs = batch_rows * head_count
    group = queries.shape[1] // head_count
    blocks = context // BLOCK
    size, parts, cuts = plan_of(n, pairs, group)
    own = size // cuts
    chunks = parts * cuts
    owners = owners_of(n, chunks)
    most = max(owners.count(o) for o in owners)
    assert group == ROWS and ROWS % blocks == 0 and width == LANES
    assert 1 + blocks <= ROWS // 2 and size % cuts == 0 and pairs % size == 0
    rows = own * group + -(-own * blocks // ROWS) * ROWS + ROWS
    vmem = pl.BlockSpec(memory_space=pltpu.VMEM)
    smem = pl.BlockSpec(memory_space=pltpu.SMEM)
    hbm = pl.BlockSpec(memory_space=pl.ANY)
    dma = pltpu.SemaphoreType.DMA
    output = pl.pallas_call(
        functools.partial(kernel, n),
        out_shape=pltpu.VMEM((pairs * group, width), jnp.bfloat16),
        in_specs=[vmem, hbm, hbm, vmem, smem, smem, smem],
        out_specs=vmem,
        scratch_shapes=[
            pltpu.VMEM((parts, size, context, width), jnp.bfloat16),
            pltpu.VMEM((parts, size, context, width), jnp.bfloat16),
            pltpu.VMEM((chunks, rows, width), jnp.bfloat16),
            pltpu.VMEM((most, n - 1, rows, width), jnp.bfloat16),
            pltpu.VMEM((chunks, ROWS, LANES), jnp.float32),
            dma((parts,)), dma((parts,)), dma((chunks,)), dma((most, n - 1)), dma((most, n - 1)), dma((chunks,)),
        ],
        compiler_params=pltpu.CompilerParams(collective_id=0, has_side_effects=True),
    )(
        queries.reshape(pairs * group, width),
        key_cache.reshape(pairs, context, width),
        value_cache.reshape(pairs, context, width),
        gate_logits,
        lengths,
        chosen.transpose(1, 2, 0),
        counts.transpose(1, 0),
    )
    return output.reshape(batch_rows, head_count * group, width)


def solution(mesh):
    return jax.shard_map(
        functools.partial(on_device, mesh.shape["seq"]),
        mesh=mesh,
        in_specs=(
            P(("grp", "batch"), "head", None),
            P(("grp", "batch"), "head", "seq", None),
            P(("grp", "batch"), "head", "seq", None),
            P(None, ("grp", "batch"), "head"),
            P(("grp", "batch")),
            P(("grp", "batch"), "head", None),
            P(("grp", "batch"), "head"),
        ),
        out_specs=P(("grp", "batch"), "head", None),
        check_vma=False,
    )
```

```python
import functools
import math

import jax
import jax.numpy as jnp
from jax import lax
from jax.experimental import pallas as pl
from jax.experimental.pallas import tpu as pltpu
from jax.sharding import PartitionSpec as P

BLOCK = 128
LANES = 128
ROWS = 8
NEG = -1e30
LOG2E = 1.0 / math.log(2.0)
MESH = pl.DeviceIdType.MESH


def owners_of(n, chunks):
    if chunks >= 2 * n and n > 2:
        return [0, 0] + [2] + [2 - c % 2 for c in range(chunks - 3)]
    return [c * n // chunks for c in range(chunks)]


def orders_of(n, owners, parts, cuts):
    first = [sum(owners[p * cuts + i] == 0 for i in range(cuts)) for p in range(parts)]
    late = sorted(range(parts), key=lambda p: first[p])
    early = sorted(range(parts), key=lambda p: -first[p])
    return [late if d in (0, n - 1) else early for d in range(n)]


def plan_of(n, pairs, group):
    size = min(pairs, LANES // group)
    parts = pairs // size
    cuts = max(2, n // parts)
    return size, parts, cuts


def kernel(
    n, q_hbm, k_hbm, v_hbm, gate_hbm, len_hbm, chosen_hbm, count_hbm, o_ref,
    q_ref, gate_ref, len_ref, chosen_ref, count_ref,
    k_buf, v_buf, msg, r_msg, gates, held_scores, held_left,
    turn_sem, in_sem, k_sem, v_sem, ms_sem, mr_sem, gs_sem, gr_sem,
):
    pairs, tokens, width = k_hbm.shape
    group = q_ref.shape[0] // pairs
    blocks = tokens // BLOCK
    heads, slots = chosen_ref.shape[:2]
    size, parts, cuts = plan_of(n, pairs, group)
    own = size // cuts
    chunks = parts * cuts
    owners = owners_of(n, chunks)
    holders = sorted(set(owners))
    rank = {c: at for at, c in enumerate(p * cuts + i for p in orders_of(n, owners, parts, cuts)[-1] for i in range(cuts))}
    owned = {o: sorted((c for c in range(chunks) if owners[c] == o), key=rank.get) for o in holders}
    most = max(len(v) for v in owned.values())
    span = own * group
    pooled_rows = -(-own * blocks // ROWS) * ROWS
    stat_at = span + pooled_rows
    half = ROWS // 2
    assert span * 2 <= LANES
    orders = orders_of(n, owners, parts, cuts)
    per_tile = ROWS // blocks
    scale = 1.0 / math.sqrt(width)
    me = lax.axis_index("seq")

    def mine(values):
        out = values[0]
        for d in range(1, n):
            if any(v != values[0] for v in values):
                out = jnp.where(me == d, values[d], out)
        return out

    part_at = [mine([orders[d][k] for d in range(n)]) for k in range(parts)]

    def load(k, hbm, buf, sem):
        return pltpu.make_async_copy(hbm.at[pl.ds(part_at[k] * size, size)], buf.at[k], sem.at[k])

    small = [
        pltpu.make_async_copy(src, dst, in_sem.at[i])
        for i, (src, dst) in enumerate([
            (q_hbm, q_ref), (len_hbm, len_ref), (chosen_hbm, chosen_ref),
            (count_hbm, count_ref), (gate_hbm, gate_ref),
        ])
    ]
    for copy in small:
        copy.start()
    queue = [(0, k_hbm, k_buf, k_sem)]
    for k in range(1, parts):
        queue += [(k, k_hbm, k_buf, k_sem), (k - 1, v_hbm, v_buf, v_sem)]
    queue.append((parts - 1, v_hbm, v_buf, v_sem))
    for item in queue:
        pl.semaphore_signal(turn_sem, 1)
        pl.semaphore_wait(turn_sem, 1)
        load(*item).start()

    barrier = pltpu.get_barrier_semaphore()
    holds = functools.reduce(jnp.logical_or, [me == o for o in holders])

    @pl.when(holds)
    def _():
        for r in range(1, n):
            pl.semaphore_signal(
                barrier, inc=1, device_id={"seq": lax.rem(me + r, n)}, device_id_type=MESH
            )

    lane = lax.broadcasted_iota(jnp.int32, (ROWS, LANES), 1)
    row = lax.broadcasted_iota(jnp.int32, (ROWS, LANES), 0)

    def gate_row(branch, first):
        pieces = []
        at = first
        while at < first + own:
            b, h = divmod(at, heads)
            run = min(heads - h, first + own - at)
            pieces.append(gate_ref[branch, b : b + 1, h * group : (h + run) * group])
            at += run
        if span < LANES:
            pieces.append(jnp.zeros((1, LANES - span), jnp.float32))
        return jax.nn.sigmoid(jnp.concatenate(pieces, axis=1))

    def chunk_of(d, at):
        return orders[d][at // cuts] * cuts + at % cuts

    goal = [mine([owners[chunk_of(d, at)] for d in range(n)]) for at in range(chunks)]
    seat = [mine([owned[owners[chunk_of(d, at)]].index(chunk_of(d, at)) for d in range(n)]) for at in range(chunks)]
    away = [mine([int(owners[chunk_of(d, at)] != d) for d in range(n)]) == 1 for at in range(chunks)]

    def send(at):
        slot = lax.rem(me - goal[at] + n, n) - 1
        return pltpu.make_async_remote_copy(
            src_ref=msg.at[at], dst_ref=r_msg.at[seat[at], slot],
            send_sem=ms_sem.at[at], recv_sem=mr_sem.at[seat[at], slot],
            device_id={"seq": goal[at]}, device_id_type=MESH,
        )

    def arrival(at, slot):
        return pltpu.make_async_remote_copy(
            src_ref=msg.at[0], dst_ref=r_msg.at[at, slot],
            send_sem=ms_sem.at[0], recv_sem=mr_sem.at[at, slot],
            device_id={"seq": lax.rem(me + 1 + slot, n)}, device_id_type=MESH,
        )

    def limit_of(k, i, j, filled):
        b, h = part_at[k] * (size // heads) + i // heads, i % heads
        block = me * blocks + j
        hits = [(chosen_ref[h, slot, b] == block) & (slot < count_ref[h, b]) for slot in range(slots)]
        return jnp.where(functools.reduce(jnp.logical_or, hits), filled, 0)

    def score(k):
        first = pl.multiple_of(part_at[k] * (size * group), size * group)
        for i in range(0, size, 2):
            rows = q_ref[pl.ds(first + i * group, 2 * group), :]
            for o in range(2):
                both = lax.dot_general(
                    rows, k_buf[k, i + o], (((1,), (1,)), ((), ())), preferred_element_type=jnp.float32
                )
                held_scores[k, i + o] = both[o * group : (o + 1) * group]

    def weigh(k):
        columns = []
        for i in range(size):
            if i % heads == 0:
                length = len_ref[part_at[k] * (size // heads) + i // heads]
                filled = [jnp.clip(length - (me * blocks + j) * BLOCK, 0, BLOCK) for j in range(blocks)]
                fills = [jnp.full((ROWS, LANES), f, jnp.int32) for f in filled]
                live = [jnp.where(lane < f, 1.0, 0.0) for f in fills]
                root = [lax.rsqrt(jnp.maximum(f, 1).astype(jnp.float32)) * scale for f in fills]
                none = [jnp.where(f > 0, 0.0, NEG) for f in fills]
            at = i % own % per_tile
            masked, stats = [], jnp.zeros((ROWS, LANES), jnp.float32)
            for j in range(blocks):
                scores = held_scores[k, i, :, j * BLOCK : (j + 1) * BLOCK]
                total = jnp.sum(scores * live[j], axis=1, keepdims=True)
                stats = jnp.where(lane == 1 + j, total * root[j] + none[j], stats)
                masked.append(jnp.where(lane < limit_of(k, i, j, filled[j]), scores, NEG))
            top = jnp.max(functools.reduce(jnp.maximum, masked), axis=1, keepdims=True)
            top = jnp.maximum(top, NEG / 10)
            weights = [jnp.exp2((m - top) * (scale * LOG2E)) for m in masked]
            weight_sum = jnp.sum(functools.reduce(jnp.add, weights), axis=1, keepdims=True)
            stats = jnp.where(lane == 0, top * scale, jnp.where(lane == 1 + blocks, weight_sum, stats))
            columns.append(stats)
            lives = [jnp.where(row == at * blocks + j, live[j], 0.0) for j in range(blocks)]
            left = jnp.concatenate([jnp.concatenate(weights, axis=1), jnp.concatenate(lives, axis=1)], axis=0)
            held_left[k, i] = left.astype(jnp.bfloat16)
        if size * group < LANES:
            columns.append(jnp.zeros((LANES - size * group, LANES), jnp.float32))
        stats = jnp.concatenate(columns, axis=0).T[:ROWS]
        high = stats.astype(jnp.bfloat16).astype(jnp.float32)
        return high, stats - high

    def gather(k, high, low):
        for cut in range(cuts):
            c = k * cuts + cut
            outs, tiles = [], []
            for i in range(cut * own, (cut + 1) * own):
                at = (i - cut * own) % per_tile
                if at == 0:
                    members = range(i, min(i + per_tile, (cut + 1) * own))
                    length_rows = jnp.zeros((ROWS, LANES), jnp.int32)
                    for m, p in enumerate(members):
                        length = len_ref[part_at[k] * (size // heads) + p // heads]
                        length_rows = jnp.where(lax.div(row, blocks) == m, length, length_rows)
                    start_rows = (me * blocks + lax.rem(row, blocks)) * BLOCK
                    filled_rows = jnp.clip(length_rows - start_rows, 0, BLOCK)
                    root_rows = lax.rsqrt(jnp.maximum(filled_rows, 1).astype(jnp.float32))
                    pooled = jnp.zeros((ROWS, width), jnp.float32)
                summed = jnp.dot(held_left[k, i], v_buf[k, i], preferred_element_type=jnp.float32)
                outs.append(summed[:group])
                pooled = pooled + summed[group:]
                if at == per_tile - 1 or i == (cut + 1) * own - 1:
                    tiles.append(pooled * root_rows)

            def turned(x, to):
                return pltpu.roll(x, (to - cut * span) % LANES, 1) if to != cut * span else x

            parted = jnp.where(lane < LANES // 2, turned(high, 0), turned(low, LANES // 2))
            msg[c] = jnp.concatenate(outs + tiles + [parted[:half]], axis=0).astype(jnp.bfloat16)

    defer = me == 0

    def meet():
        pl.semaphore_wait(barrier, jnp.where(holds, len(holders) - 1, len(holders)))

    def launch(k, when):
        for cut in range(cuts):
            c = k * cuts + cut

            @pl.when(jnp.logical_and(away[c], when))
            def _(c=c):
                send(c).start()

    for copy in small:
        copy.wait()
    load(0, k_hbm, k_buf, k_sem).wait()
    score(0)
    for c in range(chunks):
        gates[c] = jnp.where(row == 0, gate_row(1, c * own), gate_row(0, c * own))
    stats = {}
    if parts == 1:
        stats[0] = weigh(0)
    for k in range(parts):
        if k + 1 < parts:
            load(k + 1, k_hbm, k_buf, k_sem).wait()
            score(k + 1)
            if k not in stats:
                stats[k] = weigh(k)
        load(k, v_hbm, v_buf, v_sem).wait()
        gather(k, *stats[k])
        if k + 2 == parts:
            stats[k + 1] = weigh(k + 1)
        if k == 0:
            pl.when(jnp.logical_not(defer))(meet)
        launch(k, jnp.logical_not(defer))
    pl.when(defer)(meet)
    for k in range(parts):
        launch(k, defer)

    def pick(at):
        c = 0
        for o in holders:
            if at < len(owned[o]):
                c = jnp.where(me == o, owned[o][at], c)
        return c

    def has(at):
        return functools.reduce(jnp.logical_or, [me == o for o in holders if at < len(owned[o])])

    def spot(c):
        return pl.ds(pl.multiple_of(c * span, span), span)

    def deliver(rows, sem, c, to):
        return pltpu.make_async_remote_copy(
            src_ref=rows, dst_ref=rows, send_sem=sem, recv_sem=gr_sem.at[c],
            device_id={"seq": to}, device_id_type=MESH,
        )

    def share(at, i):
        to = jnp.where(i < me, i, i + 1)
        return deliver(o_ref.at[spot(pick(at))], gs_sem.at[at, i], pick(at), to)

    def finish(at):
        c = pick(at)
        here = 0
        for o in holders:
            if at < len(owned[o]):
                spots = [chunk_of(o, i) for i in range(chunks)]
                here = jnp.where(me == o, spots.index(owned[o][at]), here)
        for slot in range(n - 1):
            arrival(at, slot).wait_recv()
        halves = row[:half]
        parts_in = [r_msg.at[at, slot] for slot in range(n - 1)] + [msg.at[here]]
        all_stats = []
        for ref in parts_in:
            parted = ref[stat_at : stat_at + half, :].astype(jnp.float32)
            all_stats.append(parted + pltpu.roll(parted, LANES // 2, 1))
        top = functools.reduce(jnp.maximum, all_stats)
        block_row = (halves >= 1) & (halves <= blocks)
        block_top = jnp.max(jnp.where(block_row, top, NEG), axis=0, keepdims=True)
        top = jnp.where(halves == 0, top, block_top)
        shares = [jnp.where(halves <= blocks, jnp.exp(s - top), 0.0) for s in all_stats]
        total = functools.reduce(jnp.add, [s[:1] * x[1 + blocks : 2 + blocks] for s, x in zip(shares, all_stats)])
        blocks_in = jnp.where(block_row, functools.reduce(jnp.add, shares), 0.0)
        block_total = jnp.sum(blocks_in, axis=0, keepdims=True)
        factor = gates[c][:half] / jnp.where(halves == 0, total, block_total)
        wide = lax.broadcasted_iota(jnp.int32, (span, LANES), 1)
        tall = lax.broadcasted_iota(jnp.int32, (span, LANES), 0)
        pool_lane = lax.broadcasted_iota(jnp.int32, (pooled_rows, LANES), 1)
        pool_row = lax.broadcasted_iota(jnp.int32, (pooled_rows, LANES), 0)
        within = lax.div(pool_lane, group) == lax.div(pool_row, blocks)
        out = None
        for ref, s in zip(parts_in, shares):
            factors = s * factor
            pick_rows = jnp.where(wide == tall, factors[:1], 0.0)
            level = jnp.broadcast_to(factors[1:2], (pooled_rows, LANES))
            for j in range(1, blocks):
                level = jnp.where(lax.rem(pool_row, blocks) == j, factors[1 + j : 2 + j], level)
            level = jnp.where(within, level, 0.0)
            left = jnp.concatenate([pick_rows, level], axis=0).astype(jnp.bfloat16)[:, :span]
            term = lax.dot_general(
                left, ref[:stat_at, :], (((0,), (0,)), ((), ())), preferred_element_type=jnp.float32
            )
            out = term if out is None else out + term
        o_ref[spot(c), :] = out.astype(jnp.bfloat16)
        for i in range(n - 1):
            share(at, i).start()

    for at in range(most):

        @pl.when(has(at))
        def _(at=at):
            finish(at)

    for c in range(chunks):

        @pl.when(me != owners[c])
        def _(c=c):
            deliver(o_ref.at[c * span : (c + 1) * span], gs_sem.at[0, 0], c, owners[c]).wait_recv()

    for at in range(chunks):

        @pl.when(away[at])
        def _(at=at):
            send(at).wait_send()

    for at in range(most):

        @pl.when(has(at))
        def _(at=at):
            for i in range(n - 1):
                share(at, i).wait_send()


def on_device(n, queries, key_cache, value_cache, gate_logits, lengths, chosen, counts):
    batch_rows, head_count, context, width = key_cache.shape
    pairs = batch_rows * head_count
    group = queries.shape[1] // head_count
    blocks = context // BLOCK
    size, parts, cuts = plan_of(n, pairs, group)
    own = size // cuts
    chunks = parts * cuts
    owners = owners_of(n, chunks)
    most = max(owners.count(o) for o in owners)
    assert group == ROWS and ROWS % blocks == 0 and width == LANES
    assert 2 + blocks <= ROWS // 2 and size % cuts == 0 and pairs % size == 0 and size % head_count == 0 and size % 2 == 0
    rows = own * group + -(-own * blocks // ROWS) * ROWS + ROWS // 2
    vmem = pl.BlockSpec(memory_space=pltpu.VMEM)
    hbm = pl.BlockSpec(memory_space=pl.ANY)
    dma = pltpu.SemaphoreType.DMA
    output = pl.pallas_call(
        functools.partial(kernel, n),
        out_shape=pltpu.VMEM((pairs * group, width), jnp.bfloat16),
        in_specs=[hbm] * 7,
        out_specs=vmem,
        scratch_shapes=[
            pltpu.VMEM((pairs * group, width), jnp.bfloat16),
            pltpu.VMEM(gate_logits.shape, jnp.float32),
            pltpu.SMEM(lengths.shape, jnp.int32),
            pltpu.SMEM((head_count, chosen.shape[2], batch_rows), jnp.int32),
            pltpu.SMEM((head_count, batch_rows), jnp.int32),
            pltpu.VMEM((parts, size, context, width), jnp.bfloat16),
            pltpu.VMEM((parts, size, context, width), jnp.bfloat16),
            pltpu.VMEM((chunks, rows, width), jnp.bfloat16),
            pltpu.VMEM((most, n - 1, rows, width), jnp.bfloat16),
            pltpu.VMEM((chunks, ROWS, LANES), jnp.float32),
            pltpu.VMEM((parts, size, group, context), jnp.float32),
            pltpu.VMEM((parts, size, 2 * group, context), jnp.bfloat16),
            pltpu.SemaphoreType.REGULAR, dma((5,)), dma((parts,)), dma((parts,)), dma((chunks,)), dma((most, n - 1)), dma((most, n - 1)), dma((chunks,)),
        ],
        compiler_params=pltpu.CompilerParams(collective_id=0, has_side_effects=True),
    )(
        queries.reshape(pairs * group, width),
        key_cache.reshape(pairs, context, width),
        value_cache.reshape(pairs, context, width),
        gate_logits,
        lengths,
        chosen.transpose(1, 2, 0),
        counts.transpose(1, 0),
    )
    return output.reshape(batch_rows, head_count * group, width)


def solution(mesh):
    return jax.shard_map(
        functools.partial(on_device, mesh.shape["seq"]),
        mesh=mesh,
        in_specs=(
            P(("grp", "batch"), "head", None),
            P(("grp", "batch"), "head", "seq", None),
            P(("grp", "batch"), "head", "seq", None),
            P(None, ("grp", "batch"), "head"),
            P(("grp", "batch")),
            P(("grp", "batch"), "head", None),
            P(("grp", "batch"), "head"),
        ),
        out_specs=P(("grp", "batch"), "head", None),
        check_vma=False,
    )
```

```python
import functools
import math

import jax
import jax.numpy as jnp
from jax import lax
from jax.experimental import pallas as pl
from jax.experimental.pallas import tpu as pltpu
from jax.sharding import PartitionSpec as P

BLOCK = 128
LANES = 128
ROWS = 8
NEG = -1e30
LOG2E = 1.0 / math.log(2.0)
MESH = pl.DeviceIdType.MESH


def owners_of(n, chunks):
    if chunks >= 2 * n and n > 2:
        return [0, 0] + [2 - c % 2 for c in range(chunks - 2)]
    return [c * n // chunks for c in range(chunks)]


def orders_of(n, owners, parts, cuts):
    def held(p, d):
        return sum(owners[p * cuts + i] == d for i in range(cuts))

    return [sorted(range(parts), key=lambda p: (held(p, d), held(p, 0))) for d in range(n)]


def plan_of(n, pairs, group):
    size = min(pairs, LANES // (2 * group))
    parts = pairs // size
    cuts = max(1, n // parts)
    return size, parts, cuts


def kernel(
    n, q_hbm, k_hbm, v_hbm, gate_hbm, len_hbm, chosen_hbm, count_hbm, o_ref,
    q_ref, gate_ref, len_ref, chosen_ref, count_ref,
    k_buf, v_buf, msg, r_msg, gates, held_scores, held_left,
    turn_sem, in_sem, k_sem, v_sem, ms_sem, mr_sem, gs_sem, gr_sem,
):
    pairs, tokens, width = k_hbm.shape
    group = q_ref.shape[0] // pairs
    blocks = tokens // BLOCK
    heads, slots = chosen_ref.shape[:2]
    size, parts, cuts = plan_of(n, pairs, group)
    own = size // cuts
    chunks = parts * cuts
    owners = owners_of(n, chunks)
    holders = sorted(set(owners))
    rank = {c: at for at, c in enumerate(p * cuts + i for p in orders_of(n, owners, parts, cuts)[-1] for i in range(cuts))}
    owned = {o: sorted((c for c in range(chunks) if owners[c] == o), key=rank.get) for o in holders}
    most = max(len(v) for v in owned.values())
    span = own * group
    pooled_rows = -(-own * blocks // ROWS) * ROWS
    stat_at = span + pooled_rows
    half = ROWS // 2
    assert span * 2 <= LANES
    orders = orders_of(n, owners, parts, cuts)
    per_tile = ROWS // blocks
    scale = 1.0 / math.sqrt(width)
    me = lax.axis_index("seq")

    def mine(values):
        out = values[0]
        for d in range(1, n):
            if any(v != values[0] for v in values):
                out = jnp.where(me == d, values[d], out)
        return out

    part_at = [mine([orders[d][k] for d in range(n)]) for k in range(parts)]

    def load(k, hbm, buf, sem):
        return pltpu.make_async_copy(hbm.at[pl.ds(part_at[k] * size, size)], buf.at[k], sem.at[k])

    small = [
        pltpu.make_async_copy(src, dst, in_sem.at[i])
        for i, (src, dst) in enumerate([
            (q_hbm, q_ref), (len_hbm, len_ref), (chosen_hbm, chosen_ref),
            (count_hbm, count_ref), (gate_hbm, gate_ref),
        ])
    ]
    for copy in small:
        copy.start()
    keys = [(k, k_hbm, k_buf, k_sem) for k in range(parts)]
    values = [(k, v_hbm, v_buf, v_sem) for k in range(parts)]
    queue = [keys[0], values[0]] + keys[1:2]
    for k in range(1, parts):
        queue += keys[k + 1 : k + 2] + [values[k]]
    for item in queue:
        pl.semaphore_signal(turn_sem, 1)
        pl.semaphore_wait(turn_sem, 1)
        load(*item).start()

    barrier = pltpu.get_barrier_semaphore()
    holds = functools.reduce(jnp.logical_or, [me == o for o in holders])

    @pl.when(holds)
    def _():
        for r in range(1, n):
            pl.semaphore_signal(
                barrier, inc=1, device_id={"seq": lax.rem(me + r, n)}, device_id_type=MESH
            )

    lane = lax.broadcasted_iota(jnp.int32, (ROWS, LANES), 1)
    row = lax.broadcasted_iota(jnp.int32, (ROWS, LANES), 0)

    def gate_row(branch, first):
        pieces = []
        at = first
        while at < first + own:
            b, h = divmod(at, heads)
            run = min(heads - h, first + own - at)
            pieces.append(gate_ref[branch, b : b + 1, h * group : (h + run) * group])
            at += run
        if span < LANES:
            pieces.append(jnp.zeros((1, LANES - span), jnp.float32))
        return jax.nn.sigmoid(jnp.concatenate(pieces, axis=1))

    def chunk_of(d, at):
        return orders[d][at // cuts] * cuts + at % cuts

    goal = [mine([owners[chunk_of(d, at)] for d in range(n)]) for at in range(chunks)]
    seat = [mine([owned[owners[chunk_of(d, at)]].index(chunk_of(d, at)) for d in range(n)]) for at in range(chunks)]
    away = [mine([int(owners[chunk_of(d, at)] != d) for d in range(n)]) == 1 for at in range(chunks)]

    def send(at):
        slot = lax.rem(me - goal[at] + n, n) - 1
        return pltpu.make_async_remote_copy(
            src_ref=msg.at[at], dst_ref=r_msg.at[seat[at], slot],
            send_sem=ms_sem.at[at], recv_sem=mr_sem.at[seat[at], slot],
            device_id={"seq": goal[at]}, device_id_type=MESH,
        )

    def arrival(at, slot):
        return pltpu.make_async_remote_copy(
            src_ref=msg.at[0], dst_ref=r_msg.at[at, slot],
            send_sem=ms_sem.at[0], recv_sem=mr_sem.at[at, slot],
            device_id={"seq": lax.rem(me + 1 + slot, n)}, device_id_type=MESH,
        )

    def limit_of(k, i, j, filled):
        b, h = part_at[k] * (size // heads) + i // heads, i % heads
        block = me * blocks + j
        hits = [(chosen_ref[h, slot, b] == block) & (slot < count_ref[h, b]) for slot in range(slots)]
        return jnp.where(functools.reduce(jnp.logical_or, hits), filled, 0)

    def score(k):
        first = pl.multiple_of(part_at[k] * (size * group), size * group)
        for i in range(0, size, 2):
            rows = q_ref[pl.ds(first + i * group, 2 * group), :]
            for o in range(2):
                both = lax.dot_general(
                    rows, k_buf[k, i + o], (((1,), (1,)), ((), ())), preferred_element_type=jnp.float32
                )
                held_scores[k, i + o] = both[o * group : (o + 1) * group]

    def weigh(k):
        columns = []
        for i in range(size):
            if i % heads == 0:
                length = len_ref[part_at[k] * (size // heads) + i // heads]
                filled = [jnp.clip(length - (me * blocks + j) * BLOCK, 0, BLOCK) for j in range(blocks)]
                fills = [jnp.full((ROWS, LANES), f, jnp.int32) for f in filled]
                live = [jnp.where(lane < f, 1.0, 0.0) for f in fills]
                root = [lax.rsqrt(jnp.maximum(f, 1).astype(jnp.float32)) * scale for f in fills]
                none = [jnp.where(f > 0, 0.0, NEG) for f in fills]
            at = i % own % per_tile
            masked, stats = [], jnp.zeros((ROWS, LANES), jnp.float32)
            for j in range(blocks):
                scores = held_scores[k, i, :, j * BLOCK : (j + 1) * BLOCK]
                total = jnp.sum(scores * live[j], axis=1, keepdims=True)
                stats = jnp.where(lane == 1 + j, total * root[j] + none[j], stats)
                masked.append(jnp.where(lane < limit_of(k, i, j, filled[j]), scores, NEG))
            top = jnp.max(functools.reduce(jnp.maximum, masked), axis=1, keepdims=True)
            top = jnp.maximum(top, NEG / 10)
            weights = [jnp.exp2((m - top) * (scale * LOG2E)) for m in masked]
            weight_sum = jnp.sum(functools.reduce(jnp.add, weights), axis=1, keepdims=True)
            stats = jnp.where(lane == 0, top * scale, jnp.where(lane == 1 + blocks, weight_sum, stats))
            columns.append(stats)
            lives = [jnp.where(row == at * blocks + j, live[j], 0.0) for j in range(blocks)]
            left = jnp.concatenate([jnp.concatenate(weights, axis=1), jnp.concatenate(lives, axis=1)], axis=0)
            held_left[k, i] = left.astype(jnp.bfloat16)
        if size * group < LANES:
            columns.append(jnp.zeros((LANES - size * group, LANES), jnp.float32))
        stats = jnp.concatenate(columns, axis=0).T[:ROWS]
        high = stats.astype(jnp.bfloat16).astype(jnp.float32)
        return high, stats - high

    def gather(k, cut, high, low):
        c = k * cuts + cut
        outs, tiles = [], []
        for i in range(cut * own, (cut + 1) * own):
            at = (i - cut * own) % per_tile
            if at == 0:
                members = range(i, min(i + per_tile, (cut + 1) * own))
                length_rows = jnp.zeros((ROWS, LANES), jnp.int32)
                for m, p in enumerate(members):
                    length = len_ref[part_at[k] * (size // heads) + p // heads]
                    length_rows = jnp.where(lax.div(row, blocks) == m, length, length_rows)
                start_rows = (me * blocks + lax.rem(row, blocks)) * BLOCK
                filled_rows = jnp.clip(length_rows - start_rows, 0, BLOCK)
                root_rows = lax.rsqrt(jnp.maximum(filled_rows, 1).astype(jnp.float32))
                pooled = jnp.zeros((ROWS, width), jnp.float32)
            summed = jnp.dot(held_left[k, i], v_buf[k, i], preferred_element_type=jnp.float32)
            outs.append(summed[:group])
            pooled = pooled + summed[group:]
            if at == per_tile - 1 or i == (cut + 1) * own - 1:
                tiles.append(pooled * root_rows)

        def turned(x, to):
            return pltpu.roll(x, (to - cut * span) % LANES, 1) if to != cut * span else x

        parted = jnp.where(lane < LANES // 2, turned(high, 0), turned(low, LANES // 2))
        msg[c] = jnp.concatenate(outs + tiles + [parted[:half]], axis=0).astype(jnp.bfloat16)

    defer = me == 0

    def meet():
        pl.semaphore_wait(barrier, jnp.where(holds, len(holders) - 1, len(holders)))

    def launch(k, cut, when):
        c = k * cuts + cut

        @pl.when(jnp.logical_and(away[c], when))
        def _():
            send(c).start()

    for copy in small:
        copy.wait()
    load(0, k_hbm, k_buf, k_sem).wait()
    score(0)
    for c in range(chunks):
        gates[c] = jnp.where(row == 0, gate_row(1, c * own), gate_row(0, c * own))
    stats = {}
    stats[0] = weigh(0)
    for k in range(parts):
        if 0 < k < parts - 1:
            load(k + 1, k_hbm, k_buf, k_sem).wait()
            score(k + 1)
            stats[k] = weigh(k)
        load(k, v_hbm, v_buf, v_sem).wait()
        if k == 0:
            pl.when(jnp.logical_not(defer))(meet)
        for cut in range(cuts):
            gather(k, cut, *stats[k])
            if cut == cuts - 1 and 0 < k == parts - 2:
                stats[k + 1] = weigh(k + 1)
            launch(k, cut, jnp.logical_not(defer))
        if k == 0 and parts > 1:
            load(1, k_hbm, k_buf, k_sem).wait()
            score(1)
            if parts == 2:
                stats[1] = weigh(1)
    pl.when(defer)(meet)
    for c in range(chunks):
        launch(c // cuts, c % cuts, defer)

    def pick(at):
        c = 0
        for o in holders:
            if at < len(owned[o]):
                c = jnp.where(me == o, owned[o][at], c)
        return c

    def has(at):
        return functools.reduce(jnp.logical_or, [me == o for o in holders if at < len(owned[o])])

    def spot(c):
        return pl.ds(pl.multiple_of(c * span, span), span)

    def deliver(rows, sem, c, to):
        return pltpu.make_async_remote_copy(
            src_ref=rows, dst_ref=rows, send_sem=sem, recv_sem=gr_sem.at[c],
            device_id={"seq": to}, device_id_type=MESH,
        )

    def share(at, i):
        to = jnp.where(i < me, i, i + 1)
        return deliver(o_ref.at[spot(pick(at))], gs_sem.at[at, i], pick(at), to)

    def finish(at):
        c = pick(at)
        here = 0
        for o in holders:
            if at < len(owned[o]):
                spots = [chunk_of(o, i) for i in range(chunks)]
                here = jnp.where(me == o, spots.index(owned[o][at]), here)
        for slot in range(n - 1):
            arrival(at, slot).wait_recv()
        halves = row[:half]
        parts_in = [r_msg.at[at, slot] for slot in range(n - 1)] + [msg.at[here]]
        all_stats = []
        for ref in parts_in:
            parted = ref[stat_at : stat_at + half, :].astype(jnp.float32)
            all_stats.append(parted + pltpu.roll(parted, LANES // 2, 1))
        top = functools.reduce(jnp.maximum, all_stats)
        block_row = (halves >= 1) & (halves <= blocks)
        block_top = jnp.max(jnp.where(block_row, top, NEG), axis=0, keepdims=True)
        top = jnp.where(halves == 0, top, block_top)
        shares = [jnp.where(halves <= blocks, jnp.exp(s - top), 0.0) for s in all_stats]
        total = functools.reduce(jnp.add, [s[:1] * x[1 + blocks : 2 + blocks] for s, x in zip(shares, all_stats)])
        blocks_in = jnp.where(block_row, functools.reduce(jnp.add, shares), 0.0)
        block_total = jnp.sum(blocks_in, axis=0, keepdims=True)
        factor = gates[c][:half] / jnp.where(halves == 0, total, block_total)
        wide = lax.broadcasted_iota(jnp.int32, (span, LANES), 1)
        tall = lax.broadcasted_iota(jnp.int32, (span, LANES), 0)
        pool_lane = lax.broadcasted_iota(jnp.int32, (pooled_rows, LANES), 1)
        pool_row = lax.broadcasted_iota(jnp.int32, (pooled_rows, LANES), 0)
        within = lax.div(pool_lane, group) == lax.div(pool_row, blocks)
        out = None
        for ref, s in zip(parts_in, shares):
            factors = s * factor
            pick_rows = jnp.where(wide == tall, factors[:1], 0.0)
            level = jnp.broadcast_to(factors[1:2], (pooled_rows, LANES))
            for j in range(1, blocks):
                level = jnp.where(lax.rem(pool_row, blocks) == j, factors[1 + j : 2 + j], level)
            level = jnp.where(within, level, 0.0)
            left = jnp.concatenate([pick_rows, level], axis=0).astype(jnp.bfloat16)[:, :span]
            term = lax.dot_general(
                left, ref[:stat_at, :], (((0,), (0,)), ((), ())), preferred_element_type=jnp.float32
            )
            out = term if out is None else out + term
        o_ref[spot(c), :] = out.astype(jnp.bfloat16)
        for i in range(n - 1):
            if i == 0:
                share(at, i).start()
            else:
                pl.when(me <= i)(lambda i=i: share(at, i).start())

    for at in range(most):

        @pl.when(has(at))
        def _(at=at):
            finish(at)

    for at in range(most):
        for i in range(1, n - 1):

            @pl.when(jnp.logical_and(has(at), me > i))
            def _(at=at, i=i):
                share(at, i).start()

    for c in range(chunks):

        @pl.when(me != owners[c])
        def _(c=c):
            deliver(o_ref.at[c * span : (c + 1) * span], gs_sem.at[0, 0], c, owners[c]).wait_recv()

    for at in range(chunks):

        @pl.when(away[at])
        def _(at=at):
            send(at).wait_send()

    for at in range(most):

        @pl.when(has(at))
        def _(at=at):
            for i in range(n - 1):
                share(at, i).wait_send()


def on_device(n, queries, key_cache, value_cache, gate_logits, lengths, chosen, counts):
    batch_rows, head_count, context, width = key_cache.shape
    pairs = batch_rows * head_count
    group = queries.shape[1] // head_count
    blocks = context // BLOCK
    size, parts, cuts = plan_of(n, pairs, group)
    own = size // cuts
    chunks = parts * cuts
    owners = owners_of(n, chunks)
    most = max(owners.count(o) for o in owners)
    assert group == ROWS and ROWS % blocks == 0 and width == LANES
    assert 2 + blocks <= ROWS // 2 and size % cuts == 0 and pairs % size == 0 and size % head_count == 0 and size % 2 == 0
    rows = own * group + -(-own * blocks // ROWS) * ROWS + ROWS // 2
    vmem = pl.BlockSpec(memory_space=pltpu.VMEM)
    hbm = pl.BlockSpec(memory_space=pl.ANY)
    dma = pltpu.SemaphoreType.DMA
    output = pl.pallas_call(
        functools.partial(kernel, n),
        out_shape=pltpu.VMEM((pairs * group, width), jnp.bfloat16),
        in_specs=[hbm] * 7,
        out_specs=vmem,
        scratch_shapes=[
            pltpu.VMEM((pairs * group, width), jnp.bfloat16),
            pltpu.VMEM(gate_logits.shape, jnp.float32),
            pltpu.SMEM(lengths.shape, jnp.int32),
            pltpu.SMEM((head_count, chosen.shape[2], batch_rows), jnp.int32),
            pltpu.SMEM((head_count, batch_rows), jnp.int32),
            pltpu.VMEM((parts, size, context, width), jnp.bfloat16),
            pltpu.VMEM((parts, size, context, width), jnp.bfloat16),
            pltpu.VMEM((chunks, rows, width), jnp.bfloat16),
            pltpu.VMEM((most, n - 1, rows, width), jnp.bfloat16),
            pltpu.VMEM((chunks, ROWS, LANES), jnp.float32),
            pltpu.VMEM((parts, size, group, context), jnp.float32),
            pltpu.VMEM((parts, size, 2 * group, context), jnp.bfloat16),
            pltpu.SemaphoreType.REGULAR, dma((5,)), dma((parts,)), dma((parts,)), dma((chunks,)), dma((most, n - 1)), dma((most, n - 1)), dma((chunks,)),
        ],
        compiler_params=pltpu.CompilerParams(collective_id=0, has_side_effects=True),
    )(
        queries.reshape(pairs * group, width),
        key_cache.reshape(pairs, context, width),
        value_cache.reshape(pairs, context, width),
        gate_logits,
        lengths,
        chosen.transpose(1, 2, 0),
        counts.transpose(1, 0),
    )
    return output.reshape(batch_rows, head_count * group, width)


def solution(mesh):
    return jax.shard_map(
        functools.partial(on_device, mesh.shape["seq"]),
        mesh=mesh,
        in_specs=(
            P(("grp", "batch"), "head", None),
            P(("grp", "batch"), "head", "seq", None),
            P(("grp", "batch"), "head", "seq", None),
            P(None, ("grp", "batch"), "head"),
            P(("grp", "batch")),
            P(("grp", "batch"), "head", None),
            P(("grp", "batch"), "head"),
        ),
        out_specs=P(("grp", "batch"), "head", None),
        check_vma=False,
    )
```

```python
import functools
import math

import jax
import jax.numpy as jnp
from jax import lax
from jax.experimental import pallas as pl
from jax.experimental.pallas import tpu as pltpu
from jax.sharding import PartitionSpec as P

BLOCK = 128
LANES = 128
ROWS = 8
NEG = -1e30
LOG2E = 1.0 / math.log(2.0)
MESH = pl.DeviceIdType.MESH


def owners_of(n, chunks):
    if chunks >= 2 * n and n > 2:
        return [0, 0] + [2 - c % 2 for c in range(chunks - 2)]
    return [c * n // chunks for c in range(chunks)]


def orders_of(n, owners, parts, cuts):
    def held(p, d):
        return sum(owners[p * cuts + i] == d for i in range(cuts))

    return [sorted(range(parts), key=lambda p: (held(p, d), held(p, 0))) for d in range(n)]


def plan_of(n, pairs, group):
    size = min(pairs, LANES // (2 * group))
    parts = pairs // size
    cuts = max(1, n // parts)
    return size, parts, cuts


def kernel(
    n, q_hbm, k_hbm, v_hbm, gate_hbm, len_hbm, chosen_hbm, count_hbm, o_ref,
    q_ref, gate_ref, len_ref, chosen_ref, count_ref,
    k_buf, v_buf, msg, r_msg, gates, held_scores, held_left,
    turn_sem, in_sem, k_sem, v_sem, ms_sem, mr_sem, gs_sem, gr_sem,
):
    pairs, tokens, width = k_hbm.shape
    group = q_ref.shape[0] // pairs
    blocks = tokens // BLOCK
    heads, slots = chosen_ref.shape[:2]
    size, parts, cuts = plan_of(n, pairs, group)
    own = size // cuts
    chunks = parts * cuts
    owners = owners_of(n, chunks)
    holders = sorted(set(owners))
    rank = {c: at for at, c in enumerate(p * cuts + i for p in orders_of(n, owners, parts, cuts)[-1] for i in range(cuts))}
    owned = {o: sorted((c for c in range(chunks) if owners[c] == o), key=rank.get) for o in holders}
    most = max(len(v) for v in owned.values())
    span = own * group
    pooled_rows = -(-own * blocks // ROWS) * ROWS
    stat_at = span + pooled_rows
    half = ROWS // 2
    assert span * 2 <= LANES
    orders = orders_of(n, owners, parts, cuts)
    per_tile = ROWS // blocks
    scale = 1.0 / math.sqrt(width)
    me = lax.axis_index("seq")

    def mine(values):
        out = values[0]
        for d in range(1, n):
            if any(v != values[0] for v in values):
                out = jnp.where(me == d, values[d], out)
        return out

    part_at = [mine([orders[d][k] for d in range(n)]) for k in range(parts)]

    def load(k, hbm, buf, sem):
        return pltpu.make_async_copy(hbm.at[pl.ds(part_at[k] * size, size)], buf.at[k], sem.at[k])

    small = [
        pltpu.make_async_copy(src, dst, in_sem.at[i])
        for i, (src, dst) in enumerate([
            (q_hbm, q_ref), (len_hbm, len_ref), (chosen_hbm, chosen_ref),
            (count_hbm, count_ref), (gate_hbm, gate_ref),
        ])
    ]
    for copy in small:
        copy.start()
    keys = [(k, k_hbm, k_buf, k_sem) for k in range(parts)]
    values = [(k, v_hbm, v_buf, v_sem) for k in range(parts)]
    queue = [x for pair in zip(keys, values) for x in pair]
    for item in queue:
        pl.semaphore_signal(turn_sem, 1)
        pl.semaphore_wait(turn_sem, 1)
        load(*item).start()

    barrier = pltpu.get_barrier_semaphore()
    holds = functools.reduce(jnp.logical_or, [me == o for o in holders])

    @pl.when(holds)
    def _():
        for r in range(1, n):
            pl.semaphore_signal(
                barrier, inc=1, device_id={"seq": lax.rem(me + r, n)}, device_id_type=MESH
            )

    lane = lax.broadcasted_iota(jnp.int32, (ROWS, LANES), 1)
    row = lax.broadcasted_iota(jnp.int32, (ROWS, LANES), 0)

    def gate_row(branch, first):
        pieces = []
        at = first
        while at < first + own:
            b, h = divmod(at, heads)
            run = min(heads - h, first + own - at)
            pieces.append(gate_ref[branch, b : b + 1, h * group : (h + run) * group])
            at += run
        if span < LANES:
            pieces.append(jnp.zeros((1, LANES - span), jnp.float32))
        return jax.nn.sigmoid(jnp.concatenate(pieces, axis=1))

    def chunk_of(d, at):
        return orders[d][at // cuts] * cuts + at % cuts

    goal = [mine([owners[chunk_of(d, at)] for d in range(n)]) for at in range(chunks)]
    seat = [mine([owned[owners[chunk_of(d, at)]].index(chunk_of(d, at)) for d in range(n)]) for at in range(chunks)]
    away = [mine([int(owners[chunk_of(d, at)] != d) for d in range(n)]) == 1 for at in range(chunks)]

    def send(at):
        slot = lax.rem(me - goal[at] + n, n) - 1
        return pltpu.make_async_remote_copy(
            src_ref=msg.at[at], dst_ref=r_msg.at[seat[at], slot],
            send_sem=ms_sem.at[at], recv_sem=mr_sem.at[seat[at], slot],
            device_id={"seq": goal[at]}, device_id_type=MESH,
        )

    def arrival(at, slot):
        return pltpu.make_async_remote_copy(
            src_ref=msg.at[0], dst_ref=r_msg.at[at, slot],
            send_sem=ms_sem.at[0], recv_sem=mr_sem.at[at, slot],
            device_id={"seq": lax.rem(me + 1 + slot, n)}, device_id_type=MESH,
        )

    def limit_of(k, i, j, filled):
        b, h = part_at[k] * (size // heads) + i // heads, i % heads
        block = me * blocks + j
        hits = [(chosen_ref[h, slot, b] == block) & (slot < count_ref[h, b]) for slot in range(slots)]
        return jnp.where(functools.reduce(jnp.logical_or, hits), filled, 0)

    def score(k):
        first = pl.multiple_of(part_at[k] * (size * group), size * group)
        for i in range(0, size, 2):
            rows = q_ref[pl.ds(first + i * group, 2 * group), :]
            for o in range(2):
                both = lax.dot_general(
                    rows, k_buf[k, i + o], (((1,), (1,)), ((), ())), preferred_element_type=jnp.float32
                )
                held_scores[k, i + o] = both[o * group : (o + 1) * group]

    def weigh(k):
        columns = []
        for i in range(size):
            if i % heads == 0:
                length = len_ref[part_at[k] * (size // heads) + i // heads]
                filled = [jnp.clip(length - (me * blocks + j) * BLOCK, 0, BLOCK) for j in range(blocks)]
                fills = [jnp.full((ROWS, LANES), f, jnp.int32) for f in filled]
                live = [jnp.where(lane < f, 1.0, 0.0) for f in fills]
                root = [lax.rsqrt(jnp.maximum(f, 1).astype(jnp.float32)) * scale for f in fills]
                none = [jnp.where(f > 0, 0.0, NEG) for f in fills]
            at = i % own % per_tile
            masked, stats = [], jnp.zeros((ROWS, LANES), jnp.float32)
            for j in range(blocks):
                scores = held_scores[k, i, :, j * BLOCK : (j + 1) * BLOCK]
                total = jnp.sum(scores * live[j], axis=1, keepdims=True)
                stats = jnp.where(lane == 1 + j, total * root[j] + none[j], stats)
                masked.append(jnp.where(lane < limit_of(k, i, j, filled[j]), scores, NEG))
            top = jnp.max(functools.reduce(jnp.maximum, masked), axis=1, keepdims=True)
            top = jnp.maximum(top, NEG / 10)
            weights = [jnp.exp2((m - top) * (scale * LOG2E)) for m in masked]
            weight_sum = jnp.sum(functools.reduce(jnp.add, weights), axis=1, keepdims=True)
            stats = jnp.where(lane == 0, top * scale, jnp.where(lane == 1 + blocks, weight_sum, stats))
            columns.append(stats)
            lives = [jnp.where(row == at * blocks + j, live[j], 0.0) for j in range(blocks)]
            left = jnp.concatenate([jnp.concatenate(weights, axis=1), jnp.concatenate(lives, axis=1)], axis=0)
            held_left[k, i] = left.astype(jnp.bfloat16)
        if size * group < LANES:
            columns.append(jnp.zeros((LANES - size * group, LANES), jnp.float32))
        stats = jnp.concatenate(columns, axis=0).T[:ROWS]
        high = stats.astype(jnp.bfloat16).astype(jnp.float32)
        return high, stats - high

    def gather(k, cut, high, low):
        c = k * cuts + cut
        outs, tiles = [], []
        for i in range(cut * own, (cut + 1) * own):
            at = (i - cut * own) % per_tile
            if at == 0:
                members = range(i, min(i + per_tile, (cut + 1) * own))
                length_rows = jnp.zeros((ROWS, LANES), jnp.int32)
                for m, p in enumerate(members):
                    length = len_ref[part_at[k] * (size // heads) + p // heads]
                    length_rows = jnp.where(lax.div(row, blocks) == m, length, length_rows)
                start_rows = (me * blocks + lax.rem(row, blocks)) * BLOCK
                filled_rows = jnp.clip(length_rows - start_rows, 0, BLOCK)
                root_rows = lax.rsqrt(jnp.maximum(filled_rows, 1).astype(jnp.float32))
                pooled = jnp.zeros((ROWS, width), jnp.float32)
            summed = jnp.dot(held_left[k, i], v_buf[k, i], preferred_element_type=jnp.float32)
            outs.append(summed[:group])
            pooled = pooled + summed[group:]
            if at == per_tile - 1 or i == (cut + 1) * own - 1:
                tiles.append(pooled * root_rows)

        def turned(x, to):
            return pltpu.roll(x, (to - cut * span) % LANES, 1) if to != cut * span else x

        parted = jnp.where(lane < LANES // 2, turned(high, 0), turned(low, LANES // 2))
        msg[c] = jnp.concatenate(outs + tiles + [parted[:half]], axis=0).astype(jnp.bfloat16)

    defer = me == 0

    def meet():
        pl.semaphore_wait(barrier, jnp.where(holds, len(holders) - 1, len(holders)))

    def launch(k, cut, when):
        c = k * cuts + cut

        @pl.when(jnp.logical_and(away[c], when))
        def _():
            send(c).start()

    for copy in small:
        copy.wait()
    load(0, k_hbm, k_buf, k_sem).wait()
    score(0)
    for c in range(chunks):
        gates[c] = jnp.where(row == 0, gate_row(1, c * own), gate_row(0, c * own))
    stats = {}
    stats[0] = weigh(0)
    for k in range(parts):
        if 0 < k < parts - 1:
            load(k + 1, k_hbm, k_buf, k_sem).wait()
            score(k + 1)
            stats[k] = weigh(k)
        load(k, v_hbm, v_buf, v_sem).wait()
        if k == 0:
            pl.when(jnp.logical_not(defer))(meet)
        for cut in range(cuts):
            gather(k, cut, *stats[k])
            if cut == cuts - 1 and 0 < k == parts - 2:
                stats[k + 1] = weigh(k + 1)
            launch(k, cut, jnp.logical_not(defer))
        if k == 0 and parts > 1:
            load(1, k_hbm, k_buf, k_sem).wait()
            score(1)
            if parts == 2:
                stats[1] = weigh(1)
    pl.when(defer)(meet)
    for c in range(chunks):
        launch(c // cuts, c % cuts, defer)

    def pick(at):
        c = 0
        for o in holders:
            if at < len(owned[o]):
                c = jnp.where(me == o, owned[o][at], c)
        return c

    def has(at):
        return functools.reduce(jnp.logical_or, [me == o for o in holders if at < len(owned[o])])

    def spot(c):
        return pl.ds(pl.multiple_of(c * span, span), span)

    def deliver(rows, sem, c, to):
        return pltpu.make_async_remote_copy(
            src_ref=rows, dst_ref=rows, send_sem=sem, recv_sem=gr_sem.at[c],
            device_id={"seq": to}, device_id_type=MESH,
        )

    def share(at, i):
        to = jnp.where(i < me, i, i + 1)
        return deliver(o_ref.at[spot(pick(at))], gs_sem.at[at, i], pick(at), to)

    def finish(at):
        c = pick(at)
        here = 0
        for o in holders:
            if at < len(owned[o]):
                spots = [chunk_of(o, i) for i in range(chunks)]
                here = jnp.where(me == o, spots.index(owned[o][at]), here)
        for slot in range(n - 1):
            arrival(at, slot).wait_recv()
        halves = row[:half]
        parts_in = [r_msg.at[at, slot] for slot in range(n - 1)] + [msg.at[here]]
        all_stats = []
        for ref in parts_in:
            parted = ref[stat_at : stat_at + half, :].astype(jnp.float32)
            all_stats.append(parted + pltpu.roll(parted, LANES // 2, 1))
        top = functools.reduce(jnp.maximum, all_stats)
        block_row = (halves >= 1) & (halves <= blocks)
        block_top = jnp.max(jnp.where(block_row, top, NEG), axis=0, keepdims=True)
        top = jnp.where(halves == 0, top, block_top)
        shares = [jnp.where(halves <= blocks, jnp.exp(s - top), 0.0) for s in all_stats]
        total = functools.reduce(jnp.add, [s[:1] * x[1 + blocks : 2 + blocks] for s, x in zip(shares, all_stats)])
        blocks_in = jnp.where(block_row, functools.reduce(jnp.add, shares), 0.0)
        block_total = jnp.sum(blocks_in, axis=0, keepdims=True)
        factor = gates[c][:half] / jnp.where(halves == 0, total, block_total)
        wide = lax.broadcasted_iota(jnp.int32, (span, LANES), 1)
        tall = lax.broadcasted_iota(jnp.int32, (span, LANES), 0)
        pool_lane = lax.broadcasted_iota(jnp.int32, (pooled_rows, LANES), 1)
        pool_row = lax.broadcasted_iota(jnp.int32, (pooled_rows, LANES), 0)
        within = lax.div(pool_lane, group) == lax.div(pool_row, blocks)
        out = None
        for ref, s in zip(parts_in, shares):
            factors = s * factor
            pick_rows = jnp.where(wide == tall, factors[:1], 0.0)
            level = jnp.broadcast_to(factors[1:2], (pooled_rows, LANES))
            for j in range(1, blocks):
                level = jnp.where(lax.rem(pool_row, blocks) == j, factors[1 + j : 2 + j], level)
            level = jnp.where(within, level, 0.0)
            left = jnp.concatenate([pick_rows, level], axis=0).astype(jnp.bfloat16)[:, :span]
            term = lax.dot_general(
                left, ref[:stat_at, :], (((0,), (0,)), ((), ())), preferred_element_type=jnp.float32
            )
            out = term if out is None else out + term
        o_ref[spot(c), :] = out.astype(jnp.bfloat16)
        for i in range(n - 1):
            if i == 0:
                share(at, i).start()
            else:
                pl.when(me <= i)(lambda i=i: share(at, i).start())

    for at in range(most):

        @pl.when(has(at))
        def _(at=at):
            finish(at)

    for at in range(most):
        for i in range(1, n - 1):

            @pl.when(jnp.logical_and(has(at), me > i))
            def _(at=at, i=i):
                share(at, i).start()

    for c in range(chunks):

        @pl.when(me != owners[c])
        def _(c=c):
            deliver(o_ref.at[c * span : (c + 1) * span], gs_sem.at[0, 0], c, owners[c]).wait_recv()

    for at in range(chunks):

        @pl.when(away[at])
        def _(at=at):
            send(at).wait_send()

    for at in range(most):

        @pl.when(has(at))
        def _(at=at):
            for i in range(n - 1):
                share(at, i).wait_send()


def on_device(n, queries, key_cache, value_cache, gate_logits, lengths, chosen, counts):
    batch_rows, head_count, context, width = key_cache.shape
    pairs = batch_rows * head_count
    group = queries.shape[1] // head_count
    blocks = context // BLOCK
    size, parts, cuts = plan_of(n, pairs, group)
    own = size // cuts
    chunks = parts * cuts
    owners = owners_of(n, chunks)
    most = max(owners.count(o) for o in owners)
    assert group == ROWS and ROWS % blocks == 0 and width == LANES
    assert 2 + blocks <= ROWS // 2 and size % cuts == 0 and pairs % size == 0 and size % head_count == 0 and size % 2 == 0
    rows = own * group + -(-own * blocks // ROWS) * ROWS + ROWS // 2
    vmem = pl.BlockSpec(memory_space=pltpu.VMEM)
    hbm = pl.BlockSpec(memory_space=pl.ANY)
    dma = pltpu.SemaphoreType.DMA
    output = pl.pallas_call(
        functools.partial(kernel, n),
        out_shape=pltpu.VMEM((pairs * group, width), jnp.bfloat16),
        in_specs=[hbm] * 7,
        out_specs=vmem,
        scratch_shapes=[
            pltpu.VMEM((pairs * group, width), jnp.bfloat16),
            pltpu.VMEM(gate_logits.shape, jnp.float32),
            pltpu.SMEM(lengths.shape, jnp.int32),
            pltpu.SMEM((head_count, chosen.shape[2], batch_rows), jnp.int32),
            pltpu.SMEM((head_count, batch_rows), jnp.int32),
            pltpu.VMEM((parts, size, context, width), jnp.bfloat16),
            pltpu.VMEM((parts, size, context, width), jnp.bfloat16),
            pltpu.VMEM((chunks, rows, width), jnp.bfloat16),
            pltpu.VMEM((most, n - 1, rows, width), jnp.bfloat16),
            pltpu.VMEM((chunks, ROWS, LANES), jnp.float32),
            pltpu.VMEM((parts, size, group, context), jnp.float32),
            pltpu.VMEM((parts, size, 2 * group, context), jnp.bfloat16),
            pltpu.SemaphoreType.REGULAR, dma((5,)), dma((parts,)), dma((parts,)), dma((chunks,)), dma((most, n - 1)), dma((most, n - 1)), dma((chunks,)),
        ],
        compiler_params=pltpu.CompilerParams(collective_id=0, has_side_effects=True),
    )(
        queries.reshape(pairs * group, width),
        key_cache.reshape(pairs, context, width),
        value_cache.reshape(pairs, context, width),
        gate_logits,
        lengths,
        chosen.transpose(1, 2, 0),
        counts.transpose(1, 0),
    )
    return output.reshape(batch_rows, head_count * group, width)


def solution(mesh):
    return jax.shard_map(
        functools.partial(on_device, mesh.shape["seq"]),
        mesh=mesh,
        in_specs=(
            P(("grp", "batch"), "head", None),
            P(("grp", "batch"), "head", "seq", None),
            P(("grp", "batch"), "head", "seq", None),
            P(None, ("grp", "batch"), "head"),
            P(("grp", "batch")),
            P(("grp", "batch"), "head", None),
            P(("grp", "batch"), "head"),
        ),
        out_specs=P(("grp", "batch"), "head", None),
        check_vma=False,
    )
```
